256 devices in a mesh: row: 8 (over x, core), col: 32 (over y, z).
Axes of the slice: x: 4, y: 4, z: 8, core: 2. Of those that a mesh axis runs over, the one named last changes fastest.
Arguments:
- embeddings: bfloat16 [32768, 512], P(('row', 'col')), may hold values from -6 to 6
- sketch: bfloat16 [32768, 64], P(('row', 'col')), may hold values from -240 to 240
Outputs:
- basis: float32 [32768, 64], P(('row', 'col'))
- first_pass: float32 [32768, 64], P(('row', 'col'))
The draws below stay inside these ranges and needn't reach their ends.
All inputs are finite; a program needn't handle non-finite values.
Results may differ from the reference program's by a relative error of at most 0.00205.
Values may be sent and summed in bfloat16 or wider, within the bound.
A program may use at most 64 MiB of HBM per device.

```python
import math
import jax
import jax.numpy as jnp
from jax import lax

D = 512
R = 64
NTOTAL = 32768


def draw_sketch(key, part):
    base = jnp.clip(jax.random.normal(key, (NTOTAL, R), jnp.float32), -6.0, 6.0)
    position = jnp.arange(NTOTAL, dtype=jnp.float32) / max(NTOTAL - 1, 1)
    scale = jnp.exp(math.log(3.0) * position)[:, None]
    return (base * scale).astype(jnp.bfloat16)


def level_of(rng, extent, shards, least, high):
    level, own = 1.0, jax.random.fold_in(rng, 6)
    for axis_at, blocks in shards:
        steps = jnp.exp(jax.random.uniform(jax.random.fold_in(own, axis_at), (blocks,), jnp.float32, least / len(shards), high / len(shards)))
        level = level * jnp.repeat(steps, extent[axis_at] // blocks).reshape([-1 if axis == axis_at else 1 for axis in range(len(extent))])
    return level


def scatter_about(rng, extent, scale, bound, pieces=(), held_as=jnp.bfloat16):
    values = jax.random.normal(rng, extent, jnp.float32) * scale
    if len(pieces) > 0:
        values = level_of(rng, extent, pieces, -0.22, 0.18) * values
    return jnp.clip(values, min=-bound, max=bound).astype(held_as)


def setup_inputs(seed: int = 0) -> dict:
    key_list = jax.random.split(jax.random.key(seed), 3)
    embeddings = scatter_about(key_list[0], (NTOTAL, D), 1.0, 6.0, ((0, 256),))
    sketch = draw_sketch(jax.random.fold_in(key_list[2], 71), 0)
    return {"embeddings": embeddings, "sketch": sketch}


def reference(embeddings, sketch):
    gamma = 3.0 / D
    norms = lax.optimization_barrier(jnp.sum(jnp.square(embeddings.astype(jnp.float32)), axis=1))
    size = 1024 if NTOTAL % 1024 == 0 else NTOTAL
    blocks = embeddings.reshape(NTOTAL // size, size, D)
    norm_blocks = norms.reshape(NTOTAL // size, size)

    def one_block(pair):
        rows, row_sq = pair
        cross = lax.dot_general(rows.astype(jnp.float32), embeddings.astype(jnp.float32), (((1,), (1,)), ((), ())), preferred_element_type=jnp.float32)
        dist = row_sq[:, None] + norms[None, :] - 2.0 * cross
        tile = jnp.exp(-gamma * dist).astype(jnp.bfloat16)
        return jnp.dot(tile.astype(jnp.float32), sketch.astype(jnp.float32), preferred_element_type=jnp.float32)
    sketched = lax.map(one_block, (blocks, norm_blocks)).reshape(NTOTAL, R)
    tests = sketch.astype(jnp.float32)
    core = jnp.dot(tests.T, sketched, precision=lax.Precision.HIGHEST)
    lower = jnp.linalg.cholesky(core)
    first = jax.scipy.linalg.solve_triangular(lower, sketched.T, lower=True).T
    gram_two = jnp.dot(first.T, first, precision=lax.Precision.HIGHEST)
    lower_two = jnp.linalg.cholesky(gram_two)
    second = jax.scipy.linalg.solve_triangular(lower_two, first.T, lower=True).T
    scale = jnp.sqrt(jnp.float32(NTOTAL))
    return (second * scale, first * scale)
```

```python
import functools
import math

import jax
import jax.numpy as jnp
from jax import lax
from jax.experimental import pallas as pl
from jax.experimental.pallas import tpu as pltpu
from jax.sharding import Mesh
from jax.sharding import PartitionSpec as P

MESH = pl.DeviceIdType.MESH
AXES = ("x", "core", "y", "z")
NX, NY, NZ = 4, 4, 8
PTS, WIDTH, RANK = 128, 512, 64
PLANE = [
    (0, 0),
    (1, 0), (3, 0), (0, 1), (0, 3),
    (1, 1), (3, 1), (1, 3), (3, 3), (2, 0), (0, 2),
    (2, 1), (2, 3), (1, 2), (3, 2),
    (2, 2),
]
LINE = [0, 1, 7, 2, 6, 3, 5, 4]
PLANE_AT = {offset: at for at, offset in enumerate(PLANE)}
LINE_AT = {offset: at for at, offset in enumerate(LINE)}
N_COPIES = 96
PART = jnp.float32


def high_dot(left, right, dims):
    return lax.dot_general(
        left, right, (dims, ((), ())),
        precision=lax.Precision.HIGHEST,
        preferred_element_type=jnp.float32,
    )


def side_by_side(block):
    half = block.shape[0] // 2
    return jnp.concatenate([block[:half], block[half:]], axis=1)


def one_above_other(block):
    half = block.shape[1] // 2
    return jnp.concatenate([block[:, :half], block[:, half:]], axis=0)


def inverse_of_cholesky(sym):
    n = sym.shape[0]
    sub = lax.broadcasted_iota(jnp.int32, (n, n), 0)
    lane = lax.broadcasted_iota(jnp.int32, (n, n), 1)
    work = jnp.concatenate([sym, (sub == lane).astype(jnp.float32)], axis=1)
    tile = 8
    in_tile = lax.broadcasted_iota(jnp.int32, (tile, 2 * n), 0)
    tiles = [work[t * tile : (t + 1) * tile] for t in range(n // tile)]
    for p in range(n // tile):
        base = p * tile
        rows = tiles[p]
        below = list(range(p, n // tile))
        cols = [
            [jnp.broadcast_to(tiles[t][:, base + k : base + k + 1], (tile, 2 * n)) for t in below]
            for k in range(tile)
        ]
        done = []
        for k in range(tile):
            inv = lax.rsqrt(jnp.broadcast_to(cols[k][0][k : k + 1], (tile, 2 * n)))
            low = [c * inv for c in cols[k]]
            row = jnp.broadcast_to(rows[k : k + 1], (tile, 2 * n)) * inv
            for m in range(k + 1, tile):
                scale = jnp.broadcast_to(low[0][m : m + 1], (tile, 2 * n))
                cols[m] = [c - l * scale for c, l in zip(cols[m], low)]
            rows = jnp.where(in_tile > k, rows - low[0] * row, jnp.where(in_tile == k, row, rows))
            done.append((low, row))
        tiles[p] = rows
        for t in range(p + 1, n // tile):
            acc = tiles[t]
            for low, row in done:
                acc = acc - low[t - p] * row
            tiles[t] = acc
    return jnp.concatenate(tiles, axis=0)[:, n:]


def kernel(
    e_hbm, s_ref, basis_ref, first_ref,
    ea, eb, sd, naf, nbf, y_acc, rs_out, rs_in, gram, g_part, g_x, g_y, g_z, g_sum, inv_pair,
    load_sem, send_sem, recv_sem,
):
    me = {axis: lax.axis_index(axis) for axis in AXES}
    core = me["core"]
    coef = 3.0 / WIDTH * math.log2(math.e)

    def shift(axis, by, size):
        return lax.rem(me[axis] + by, size)

    def plane_peer(dx, dy):
        return {"x": shift("x", dx, NX), "y": shift("y", dy, NY)}

    partner = {"core": 1 - core}
    left, right = plane_peer(NX - 1, 0), plane_peer(1, 0)
    down, up = plane_peer(0, NY - 1), plane_peer(0, 1)
    below, above = {"z": shift("z", NZ - 1, NZ)}, {"z": shift("z", 1, NZ)}

    copies = {}

    def send(key, src, dst, to):
        at = len(copies)
        copy = pltpu.make_async_remote_copy(
            src_ref=src, dst_ref=dst,
            send_sem=send_sem.at[at], recv_sem=recv_sem.at[at],
            device_id=to, device_id_type=MESH,
        )
        copy.start()
        assert key not in copies
        copies[key] = copy

    def arrived(*keys):
        for key in keys:
            copies[key].wait_recv()

    own_a = pltpu.make_async_copy(e_hbm, ea.at[0, pl.ds(0, PTS)], load_sem.at[0])
    own_b = pltpu.make_async_copy(e_hbm, eb.at[pl.ds(0, PTS)], load_sem.at[1])
    own_b.start()
    own_a.start()

    barrier = pltpu.get_barrier_semaphore()
    peers = [partner]
    peers += [plane_peer(dx, dy) for dx, dy in PLANE[1:]]
    peers += [{"z": shift("z", dz, NZ)} for dz in range(1, NZ)]
    for peer in peers:
        pl.semaphore_signal(barrier, inc=1, device_id=peer, device_id_type=MESH)

    own_b.wait()
    own_a.wait()
    points = eb[0:PTS].astype(jnp.float32)
    norms = high_dot(jnp.ones((16, WIDTH), jnp.float32), points * points, ((1,), (1,)))
    one = norms.astype(jnp.bfloat16).astype(jnp.float32)
    two = (norms - one).astype(jnp.bfloat16).astype(jnp.float32)
    three = norms - one - two
    at_row = lax.broadcasted_iota(jnp.int32, norms.shape, 0)
    split = jnp.where(at_row == 0, one, jnp.where(at_row == 1, two, three))
    sd[0, 0:RANK, 0:PTS] = s_ref[...].astype(jnp.float32).T.astype(jnp.bfloat16)
    sd[0, RANK : RANK + 16, 0:PTS] = split.astype(jnp.bfloat16)
    pl.semaphore_wait(barrier, len(peers))

    def send_plane(offset, rows, to, by):
        dx, dy = offset
        there = ((dx + by[0]) % NX, (dy + by[1]) % NY)
        lo, hi = rows
        send(
            (there, lo),
            eb.at[pl.ds(PLANE_AT[offset] * PTS + lo, hi - lo)],
            eb.at[pl.ds(PLANE_AT[there] * PTS + lo, hi - lo)],
            to,
        )

    def to_left(offset, lo, hi):
        send_plane(offset, (lo, hi), left, (1, 0))

    def to_right(offset, lo, hi):
        send_plane(offset, (lo, hi), right, (-1, 0))

    def to_down(offset, lo, hi):
        send_plane(offset, (lo, hi), down, (0, 1))

    def to_up(offset, lo, hi):
        send_plane(offset, (lo, hi), up, (0, -1))

    def send_line(offset, lo, hi, to, by, side):
        there = (offset + by) % NZ
        a, b = LINE_AT[offset], LINE_AT[there]
        if side:
            send(("side", there), sd.at[a, :, pl.ds(0, PTS)], sd.at[b, :, pl.ds(0, PTS)], to)
        send(("line", there, lo), ea.at[a, pl.ds(lo, hi - lo)], ea.at[b, pl.ds(lo, hi - lo)], to)

    def send_partner(offset):
        a = LINE_AT[offset]
        send(("pside", offset), sd.at[a, :, pl.ds(0, PTS)], sd.at[a, :, pl.ds(PTS, PTS)], partner)
        send(("pline", offset), ea.at[a, pl.ds(0, PTS)], ea.at[a, pl.ds(PTS, PTS)], partner)

    def norms_of_line(offset):
        arrived(("pside", offset), ("pline", offset))
        a = LINE_AT[offset]
        parts = sd[a, RANK : RANK + 16, :].astype(jnp.float32)
        total = (parts[0:1] + parts[1:2]) + parts[2:3]
        naf[a] = jnp.broadcast_to(total * coef, (8, 2 * PTS))

    def norms_of_plane(lo, hi):
        for at in range(lo, hi):
            block = eb[at * PTS : (at + 1) * PTS].astype(jnp.float32)
            total = jnp.sum(block * block, axis=1, keepdims=True) * coef
            nbf[at * PTS : (at + 1) * PTS] = jnp.broadcast_to(total, (PTS, 128))

    def multiply(lines, lo, hi, first=False):
        at = lo
        while at < hi:
            blocks = min(4, hi - at)
            rows = slice(at * PTS, (at + blocks) * PTS)
            total = None
            for a in lines:
                cross = lax.dot_general(
                    eb[rows], ea[a], (((1,), (1,)), ((), ())), preferred_element_type=jnp.float32
                )
                side = jnp.concatenate([nbf[rows], nbf[rows]], axis=1)
                tile = jnp.exp2(cross * (2.0 * coef) - naf[a, 0:1] - side).astype(jnp.bfloat16)
                term = lax.dot_general(
                    tile, sd[a, 0:RANK], (((1,), (1,)), ((), ())), preferred_element_type=jnp.float32
                )
                total = term if total is None else total + term
            y_acc[rows] = total if first else y_acc[rows] + total
            at += blocks

    own = (0, 0)
    to_left(own, 0, PTS)
    to_right(own, 0, PTS)
    to_down(own, 0, PTS)
    to_up(own, 0, PTS)
    send_line(0, 0, PTS, below, 1, True)
    send_line(0, 0, PTS, above, -1, True)
    send_partner(0)
    norms_of_plane(0, 1)
    norms_of_line(0)

    arrived(("side", 1), ("line", 1, 0))
    send_line(1, 0, PTS, below, 1, True)
    send_partner(1)
    arrived(("side", 7), ("line", 7, 0))
    send_line(7, 0, PTS, above, -1, True)
    send_partner(7)
    arrived(((1, 0), 0))
    to_down((1, 0), 0, 64)
    to_up((1, 0), 0, 64)
    to_left((1, 0), 0, 32)
    arrived(((3, 0), 0))
    to_down((3, 0), 0, 64)
    to_up((3, 0), 0, 64)
    to_right((3, 0), 32, 64)
    arrived(((0, 1), 0))
    to_left((0, 1), 64, 128)
    to_right((0, 1), 64, 128)
    to_down((0, 1), 64, 96)
    arrived(((0, 3), 0))
    to_left((0, 3), 64, 128)
    to_right((0, 3), 64, 128)
    to_up((0, 3), 96, 128)
    to_left((1, 0), 64, 128)
    to_down((0, 1), 0, 64)
    norms_of_plane(1, 5)
    multiply([0], 0, 5, first=True)
    norms_of_line(1)
    norms_of_line(7)
    multiply([1, 2], 0, 5)

    arrived(("side", 2), ("line", 2, 0))
    send_line(2, 0, PTS, below, 1, True)
    send_partner(2)
    arrived(("side", 6), ("line", 6, 0))
    send_line(6, 0, PTS, above, -1, True)
    send_partner(6)
    arrived(((2, 0), 0), ((2, 0), 32))
    to_down((2, 0), 0, 64)
    to_up((2, 0), 0, 64)
    arrived(((0, 2), 64), ((0, 2), 96))
    to_left((0, 2), 64, 128)
    to_right((0, 2), 64, 128)
    arrived(((1, 1), 0))
    to_down((1, 1), 0, 64)
    arrived(((3, 3), 0))
    to_up((3, 3), 0, 64)
    arrived(((1, 1), 64))
    to_left((1, 1), 64, 128)
    arrived(((3, 3), 64))
    to_right((3, 3), 64, 128)
    arrived(((3, 1), 0), ((3, 1), 64), ((1, 3), 0), ((1, 3), 64), ((2, 0), 64), ((0, 2), 0))
    norms_of_plane(5, 11)
    multiply([0, 1, 2], 5, 11, first=True)
    norms_of_line(2)
    norms_of_line(6)
    multiply([3, 4], 0, 11)

    arrived(("side", 3), ("line", 3, 0))
    send_line(3, 0, 64, below, 1, True)
    send_partner(3)
    arrived(("side", 5), ("line", 5, 0))
    send_line(5, 64, 128, above, -1, False)
    send_partner(5)
    arrived(((2, 3), 0))
    to_up((2, 3), 0, 64)
    arrived(((3, 2), 64))
    to_right((3, 2), 64, 128)
    arrived(((2, 1), 0), ((2, 1), 64), ((2, 3), 64), ((1, 2), 0), ((1, 2), 64), ((3, 2), 0))
    norms_of_plane(11, 15)
    multiply([0, 1, 2, 3, 4], 11, 15, first=True)
    arrived(("side", 4), ("line", 4, 0), ("line", 4, 64))
    send_partner(4)
    norms_of_line(3)
    norms_of_line(5)
    multiply([5, 6], 0, 15)

    arrived(((2, 2), 0), ((2, 2), 64))
    norms_of_plane(15, 16)
    multiply([0, 1, 2, 3, 4, 5, 6], 15, 16, first=True)
    norms_of_line(4)
    for lo in range(0, 16, 4):
        multiply([7], lo, lo + 4)
        for at in range(lo, lo + 4):
            rs_out[at] = side_by_side(y_acc[at * PTS : (at + 1) * PTS]).astype(PART)
        for at in range(max(lo, 1), lo + 4):
            dx, dy = PLANE[at]
            there = PLANE_AT[(-dx % NX, -dy % NY)]
            send(("part", there), rs_out.at[at], rs_in.at[there], plane_peer(dx, dy))

    total = side_by_side(y_acc[0:PTS])
    for at in range(1, 16):
        arrived(("part", at))
        total = total + rs_in[at].astype(jnp.float32)
    sketched = one_above_other(total)
    tests = s_ref[...].astype(jnp.float32)
    products = high_dot(
        jnp.concatenate([tests, sketched], axis=1),
        jnp.concatenate([sketched, tests], axis=1),
        ((0,), (0,)),
    )
    gram[0] = side_by_side(0.5 * (products[:RANK, :RANK] + products[RANK:, RANK:]))
    gram[1] = side_by_side(products[RANK:, :RANK])

    send("core", gram.at[1 - core], g_part, partner)
    arrived("core")
    g_sum[0] = gram[core] + g_part[...]
    for stage, axis, size, landing in ((0, "x", NX, g_x), (1, "y", NY, g_y), (2, "z", NZ, g_z)):
        for by in range(1, size):
            send((axis, by), g_sum.at[stage], landing.at[by - 1], {axis: shift(axis, by, size)})
        value = g_sum[stage]
        for by in range(1, size):
            arrived((axis, by))
            value = value + landing[by - 1]
        if stage < 2:
            g_sum[stage + 1] = value
    mine = one_above_other(value)
    inv = inverse_of_cholesky(mine)
    inv_pair[core] = side_by_side(inv)
    send("inv", inv_pair.at[core], inv_pair.at[core], partner)
    arrived("inv")
    scale = math.sqrt(PTS * 256)
    low = one_above_other(inv_pair[0])
    low_two = one_above_other(inv_pair[1])
    first_ref[...] = high_dot(sketched, low, ((1,), (1,))) * scale
    basis_ref[...] = high_dot(sketched, low_two, ((1,), (1,))) * scale
    for copy in copies.values():
        copy.wait_send()
    assert len(copies) <= N_COPIES


def per_device(embeddings, sketch):
    vmem = pl.BlockSpec(memory_space=pltpu.VMEM)
    out = jax.ShapeDtypeStruct((PTS, RANK), jnp.float32)
    packed = (RANK // 2, 2 * RANK)
    basis, first = pl.pallas_call(
        kernel,
        out_shape=(out, out),
        in_specs=[pl.BlockSpec(memory_space=pl.ANY), vmem],
        out_specs=(vmem, vmem),
        scratch_shapes=[
            pltpu.VMEM((NZ, 2 * PTS, WIDTH), jnp.bfloat16),
            pltpu.VMEM((16 * PTS, WIDTH), jnp.bfloat16),
            pltpu.VMEM((NZ, RANK + 16, 2 * PTS), jnp.bfloat16),
            pltpu.VMEM((NZ, 8, 2 * PTS), jnp.float32),
            pltpu.VMEM((16 * PTS, 128), jnp.float32),
            pltpu.VMEM((16 * PTS, RANK), jnp.float32),
            pltpu.VMEM((16, PTS // 2, 2 * RANK), PART),
            pltpu.VMEM((16, PTS // 2, 2 * RANK), PART),
            pltpu.VMEM((2, *packed), jnp.float32),
            pltpu.VMEM(packed, jnp.float32),
            pltpu.VMEM((NX - 1, *packed), jnp.float32),
            pltpu.VMEM((NY - 1, *packed), jnp.float32),
            pltpu.VMEM((NZ - 1, *packed), jnp.float32),
            pltpu.VMEM((3, *packed), jnp.float32),
            pltpu.VMEM((2, *packed), jnp.float32),
            pltpu.SemaphoreType.DMA((2,)),
            pltpu.SemaphoreType.DMA((N_COPIES,)),
            pltpu.SemaphoreType.DMA((N_COPIES,)),
        ],
        compiler_params=pltpu.CompilerParams(
            collective_id=0, has_side_effects=True, vmem_limit_bytes=40 << 20
        ),
        name="nystrom",
    )(embeddings, sketch)
    return basis, first


def solution(mesh):
    torus = Mesh(mesh.devices.reshape(NX, 2, NY, NZ), AXES)
    spec = P(AXES, None)
    return jax.shard_map(
        per_device, mesh=torus, in_specs=(spec, spec), out_specs=(spec, spec), check_vma=False
    )
```

```python
import functools
import math

import jax
import jax.numpy as jnp
from jax import lax
from jax.experimental import pallas as pl
from jax.experimental.pallas import tpu as pltpu
from jax.sharding import Mesh
from jax.sharding import PartitionSpec as P

MESH = pl.DeviceIdType.MESH
AXES = ("x", "core", "y", "z")
NX, NY, NZ = 4, 4, 8
PTS, WIDTH, RANK = 128, 512, 64
PLANE = [
    (0, 0),
    (1, 0), (3, 0), (0, 1), (0, 3),
    (1, 1), (3, 1), (1, 3), (3, 3), (2, 0), (0, 2),
    (2, 1), (2, 3), (1, 2), (3, 2),
    (2, 2),
]
LINE = [0, 1, 7, 2, 6, 3, 5, 4]
PLANE_AT = {offset: at for at, offset in enumerate(PLANE)}
LINE_AT = {offset: at for at, offset in enumerate(LINE)}
N_COPIES = 128
PART = jnp.float32


def high_dot(left, right, dims):
    return lax.dot_general(
        left, right, (dims, ((), ())),
        precision=lax.Precision.HIGHEST,
        preferred_element_type=jnp.float32,
    )


def side_by_side(block):
    half = block.shape[0] // 2
    return jnp.concatenate([block[:half], block[half:]], axis=1)


def one_above_other(block):
    half = block.shape[1] // 2
    return jnp.concatenate([block[:, :half], block[:, half:]], axis=0)


def inverse_of_cholesky(sym):
    n = sym.shape[0]
    sub = lax.broadcasted_iota(jnp.int32, (n, n), 0)
    lane = lax.broadcasted_iota(jnp.int32, (n, n), 1)
    work = jnp.concatenate([sym, (sub == lane).astype(jnp.float32)], axis=1)
    tile = 8
    in_tile = lax.broadcasted_iota(jnp.int32, (tile, 2 * n), 0)
    tiles = [work[t * tile : (t + 1) * tile] for t in range(n // tile)]
    for p in range(n // tile):
        base = p * tile
        rows = tiles[p]
        below = list(range(p, n // tile))
        cols = [
            [jnp.broadcast_to(tiles[t][:, base + k : base + k + 1], (tile, 2 * n)) for t in below]
            for k in range(tile)
        ]
        done = []
        for k in range(tile):
            inv = lax.rsqrt(jnp.broadcast_to(cols[k][0][k : k + 1], (tile, 2 * n)))
            low = [c * inv for c in cols[k]]
            row = jnp.broadcast_to(rows[k : k + 1], (tile, 2 * n)) * inv
            for m in range(k + 1, tile):
                scale = jnp.broadcast_to(low[0][m : m + 1], (tile, 2 * n))
                cols[m] = [c - l * scale for c, l in zip(cols[m], low)]
            rows = jnp.where(in_tile > k, rows - low[0] * row, jnp.where(in_tile == k, row, rows))
            done.append((low, row))
        tiles[p] = rows
        for t in range(p + 1, n // tile):
            acc = tiles[t]
            for low, row in done:
                acc = acc - low[t - p] * row
            tiles[t] = acc
    return jnp.concatenate(tiles, axis=0)[:, n:]


def kernel(
    e_hbm, s_hbm, both_ref,
    ea, eb, sd, naf, nbf, y_acc, tests_ref, rs_out, rs_in, gram, g_part, g_x, g_y, g_z, g_sum, inv_pair,
    load_sem, send_sem, recv_sem,
):
    me = {axis: lax.axis_index(axis) for axis in AXES}
    core = me["core"]
    coef = 3.0 / WIDTH * math.log2(math.e)

    def shift(axis, by, size):
        return lax.rem(me[axis] + by, size)

    def plane_peer(dx, dy):
        return {"x": shift("x", dx, NX), "y": shift("y", dy, NY)}

    partner = {"core": 1 - core}
    left, right = plane_peer(NX - 1, 0), plane_peer(1, 0)
    down, up = plane_peer(0, NY - 1), plane_peer(0, 1)
    below, above = {"z": shift("z", NZ - 1, NZ)}, {"z": shift("z", 1, NZ)}

    copies = {}

    def send(key, src, dst, to):
        at = len(copies)
        copy = pltpu.make_async_remote_copy(
            src_ref=src, dst_ref=dst,
            send_sem=send_sem.at[at], recv_sem=recv_sem.at[at],
            device_id=to, device_id_type=MESH,
        )
        copy.start()
        assert key not in copies
        copies[key] = copy

    def arrived(*keys):
        for key in keys:
            copies[key].wait_recv()

    loads = [
        pltpu.make_async_copy(e_hbm, eb.at[pl.ds(0, PTS)], load_sem.at[0]),
        pltpu.make_async_copy(s_hbm, sd.at[0, pl.ds(0, RANK), pl.ds(0, PTS)], load_sem.at[1]),
        pltpu.make_async_copy(e_hbm, ea.at[0, pl.ds(0, PTS)], load_sem.at[2]),
    ]
    for load in loads:
        load.start()
    barrier = pltpu.get_barrier_semaphore()
    peers = [partner, left, right, down, up, below, above, plane_peer(2, 0), plane_peer(0, 2)]
    for peer in peers:
        pl.semaphore_signal(barrier, inc=1, device_id=peer, device_id_type=MESH)
    for load in loads:
        load.wait()
    points = eb[0:PTS].astype(jnp.float32)
    norms = high_dot(jnp.ones((16, WIDTH), jnp.float32), points * points, ((1,), (1,)))
    one = norms.astype(jnp.bfloat16).astype(jnp.float32)
    two = (norms - one).astype(jnp.bfloat16).astype(jnp.float32)
    three = norms - one - two
    at_row = lax.broadcasted_iota(jnp.int32, norms.shape, 0)
    split = jnp.where(at_row == 0, one, jnp.where(at_row == 1, two, three))
    sd[0, RANK : RANK + 16, 0:PTS] = split.astype(jnp.bfloat16)
    tests_ref[...] = sd[0, 0:RANK, 0:PTS].astype(jnp.float32).T
    pl.semaphore_wait(barrier, len(peers))

    def send_plane(offset, rows, to, by):
        dx, dy = offset
        there = ((dx + by[0]) % NX, (dy + by[1]) % NY)
        lo, hi = rows
        send(
            (there, lo),
            eb.at[pl.ds(PLANE_AT[offset] * PTS + lo, hi - lo)],
            eb.at[pl.ds(PLANE_AT[there] * PTS + lo, hi - lo)],
            to,
        )

    def to_left(offset, lo, hi):
        send_plane(offset, (lo, hi), left, (1, 0))

    def to_right(offset, lo, hi):
        send_plane(offset, (lo, hi), right, (-1, 0))

    def to_down(offset, lo, hi):
        send_plane(offset, (lo, hi), down, (0, 1))

    def to_up(offset, lo, hi):
        send_plane(offset, (lo, hi), up, (0, -1))

    def send_line(offset, lo, hi, to, by, side):
        there = (offset + by) % NZ
        a, b = LINE_AT[offset], LINE_AT[there]
        if side:
            send(("side", there), sd.at[a, :, pl.ds(0, PTS)], sd.at[b, :, pl.ds(0, PTS)], to)
        send(("line", there, lo), ea.at[a, pl.ds(lo, hi - lo)], ea.at[b, pl.ds(lo, hi - lo)], to)

    def send_partner(offset):
        a = LINE_AT[offset]
        send(("pside", offset), sd.at[a, :, pl.ds(0, PTS)], sd.at[a, :, pl.ds(PTS, PTS)], partner)
        send(("pline", offset), ea.at[a, pl.ds(0, PTS)], ea.at[a, pl.ds(PTS, PTS)], partner)

    def norms_of_line(offset):
        arrived(("pside", offset), ("pline", offset))
        a = LINE_AT[offset]
        parts = sd[a, RANK : RANK + 16, :].astype(jnp.float32)
        total = (parts[0:1] + parts[1:2]) + parts[2:3]
        naf[a] = jnp.broadcast_to(total * coef, (8, 2 * PTS))

    def norms_of_plane(lo, hi):
        for at in range(lo, hi):
            block = eb[at * PTS : (at + 1) * PTS].astype(jnp.float32)
            total = jnp.sum(block * block, axis=1, keepdims=True) * coef
            nbf[at * PTS : (at + 1) * PTS] = jnp.broadcast_to(total, (PTS, 128))

    def multiply(lines, lo, hi, first=False):
        at = lo
        while at < hi:
            blocks = min(4, hi - at)
            rows = slice(at * PTS, (at + blocks) * PTS)
            total = None
            for a in lines:
                cross = lax.dot_general(
                    eb[rows], ea[a], (((1,), (1,)), ((), ())), preferred_element_type=jnp.float32
                )
                side = jnp.concatenate([nbf[rows], nbf[rows]], axis=1)
                tile = jnp.exp2(cross * (2.0 * coef) - naf[a, 0:1] - side).astype(jnp.bfloat16)
                term = lax.dot_general(
                    tile, sd[a, 0:RANK], (((1,), (1,)), ((), ())), preferred_element_type=jnp.float32
                )
                total = term if total is None else total + term
            y_acc[rows] = total if first else y_acc[rows] + total
            at += blocks

    def across(axis, lo, hi):
        there, to = ((2, 0), plane_peer(2, 0)) if axis == "x" else ((0, 2), plane_peer(0, 2))
        send_plane((0, 0), (lo, hi), to, there)

    def line_on(offset, lo, hi, to, by, side=None):
        arrived(*([("side", offset)] if lo == 0 else []), ("line", offset, lo))
        send_line(offset, lo, hi, to, by, (lo == 0) if side is None else side)

    own = (0, 0)
    send_line(0, 0, 64, below, 1, True)
    send_line(0, 0, 64, above, -1, True)
    to_left(own, 0, 64)
    to_right(own, 0, 64)
    to_down(own, 64, 128)
    to_up(own, 64, 128)
    across("x", 0, 64)
    across("y", 64, 128)
    send_line(0, 64, 128, below, 1, False)
    send_line(0, 64, 128, above, -1, False)
    to_left(own, 64, 128)
    to_right(own, 64, 128)
    to_down(own, 0, 64)
    to_up(own, 0, 64)
    send_partner(0)
    norms_of_plane(0, 1)
    norms_of_line(0)
    multiply([0], 0, 1, first=True)

    line_on(1, 0, 64, below, 1)
    line_on(7, 0, 64, above, -1)
    arrived(((1, 0), 0))
    to_down((1, 0), 0, 64)
    to_up((1, 0), 0, 64)
    arrived(((3, 0), 0))
    to_down((3, 0), 0, 64)
    to_up((3, 0), 0, 64)
    arrived(((0, 1), 64))
    to_left((0, 1), 64, 128)
    to_right((0, 1), 64, 128)
    arrived(((0, 3), 64))
    to_left((0, 3), 64, 128)
    to_right((0, 3), 64, 128)
    line_on(1, 64, 128, below, 1)
    send_partner(1)
    line_on(7, 64, 128, above, -1)
    send_partner(7)
    arrived(((2, 0), 0))
    to_down((2, 0), 0, 64)
    to_up((2, 0), 0, 64)
    arrived(((0, 2), 64))
    to_left((0, 2), 64, 128)
    to_right((0, 2), 64, 128)
    arrived(((1, 0), 64))
    to_left((1, 0), 64, 128)
    arrived(((0, 1), 0))
    to_down((0, 1), 0, 64)
    arrived(((3, 0), 64), ((0, 3), 0))
    norms_of_plane(1, 5)
    multiply([0], 1, 5, first=True)
    norms_of_line(1)
    norms_of_line(7)
    multiply([1, 2], 0, 5)

    line_on(2, 0, 64, below, 1)
    line_on(6, 0, 64, above, -1)
    arrived(((1, 1), 0))
    to_down((1, 1), 0, 64)
    arrived(((3, 3), 0))
    to_up((3, 3), 0, 64)
    arrived(((1, 1), 64))
    to_left((1, 1), 64, 128)
    arrived(((3, 3), 64))
    to_right((3, 3), 64, 128)
    line_on(2, 64, 128, below, 1)
    send_partner(2)
    line_on(6, 64, 128, above, -1)
    send_partner(6)
    arrived(((2, 3), 0))
    to_up((2, 3), 0, 64)
    arrived(((3, 2), 64))
    to_right((3, 2), 64, 128)
    arrived(((3, 1), 0), ((3, 1), 64), ((1, 3), 0), ((1, 3), 64), ((2, 0), 64), ((0, 2), 0))
    norms_of_plane(5, 11)
    multiply([0, 1, 2], 5, 11, first=True)
    norms_of_line(2)
    norms_of_line(6)
    multiply([3, 4], 0, 11)

    line_on(3, 0, 64, below, 1)
    arrived(("side", 5), ("line", 5, 0), ("line", 5, 64))
    send_line(5, 64, 128, above, -1, False)
    send_partner(5)
    arrived(("line", 3, 64))
    send_partner(3)
    arrived(((2, 1), 0), ((2, 1), 64), ((2, 3), 64), ((1, 2), 0), ((1, 2), 64), ((3, 2), 0), ((2, 2), 0), ((2, 2), 64))
    norms_of_plane(11, 16)
    multiply([0, 1, 2, 3, 4], 11, 16, first=True)
    norms_of_line(3)
    norms_of_line(5)
    multiply([5, 6], 8, 16)
    arrived(("side", 4), ("line", 4, 0), ("line", 4, 64))
    send_partner(4)
    multiply([5, 6], 0, 8)

    norms_of_line(4)
    for lo in (12, 8, 4, 0):
        multiply([7], lo, lo + 4)
        for at in reversed(range(max(lo, 1), lo + 4)):
            rs_out[at] = side_by_side(y_acc[at * PTS : (at + 1) * PTS]).astype(PART)
        for at in reversed(range(max(lo, 1), lo + 4)):
            dx, dy = PLANE[at]
            there = PLANE_AT[(-dx % NX, -dy % NY)]
            send(("part", there), rs_out.at[at], rs_in.at[there], plane_peer(dx, dy))

    total = side_by_side(y_acc[0:PTS])
    for at in range(1, 16):
        arrived(("part", at))
        total = total + rs_in[at].astype(jnp.float32)
    sketched = one_above_other(total)
    tests = tests_ref[...]
    products = high_dot(
        jnp.concatenate([tests, sketched], axis=1),
        jnp.concatenate([sketched, tests], axis=1),
        ((0,), (0,)),
    )
    gram[0] = side_by_side(0.5 * (products[:RANK, :RANK] + products[RANK:, RANK:]))
    gram[1] = side_by_side(products[RANK:, :RANK])

    send("core", gram.at[1 - core], g_part, partner)
    arrived("core")
    g_sum[0] = gram[core] + g_part[...]
    for stage, axis, size, landing in ((0, "x", NX, g_x), (1, "y", NY, g_y), (2, "z", NZ, g_z)):
        for by in range(1, size):
            send((axis, by), g_sum.at[stage], landing.at[by - 1], {axis: shift(axis, by, size)})
        value = g_sum[stage]
        for by in range(1, size):
            arrived((axis, by))
            value = value + landing[by - 1]
        if stage < 2:
            g_sum[stage + 1] = value
    mine = one_above_other(value)
    inv = inverse_of_cholesky(mine)
    inv_pair[core] = side_by_side(inv)
    send("inv", inv_pair.at[core], inv_pair.at[core], partner)
    arrived("inv")
    scale = math.sqrt(PTS * 256)
    low = one_above_other(inv_pair[0])
    low_two = one_above_other(inv_pair[1])
    both_ref[...] = high_dot(jnp.concatenate([low_two, low], axis=0), sketched, ((1,), (1,))) * scale
    for copy in copies.values():
        copy.wait_send()
    assert len(copies) <= N_COPIES


def per_device(embeddings, sketch):
    vmem = pl.BlockSpec(memory_space=pltpu.VMEM)
    packed = (RANK // 2, 2 * RANK)
    both = pl.pallas_call(
        kernel,
        out_shape=jax.ShapeDtypeStruct((2 * RANK, PTS), jnp.float32),
        in_specs=[pl.BlockSpec(memory_space=pl.ANY)] * 2,
        out_specs=vmem,
        scratch_shapes=[
            pltpu.VMEM((NZ, 2 * PTS, WIDTH), jnp.bfloat16),
            pltpu.VMEM((16 * PTS, WIDTH), jnp.bfloat16),
            pltpu.VMEM((NZ, RANK + 16, 2 * PTS), jnp.bfloat16),
            pltpu.VMEM((NZ, 8, 2 * PTS), jnp.float32),
            pltpu.VMEM((16 * PTS, 128), jnp.float32),
            pltpu.VMEM((16 * PTS, RANK), jnp.float32),
            pltpu.VMEM((PTS, RANK), jnp.float32),
            pltpu.VMEM((16, PTS // 2, 2 * RANK), PART),
            pltpu.VMEM((16, PTS // 2, 2 * RANK), PART),
            pltpu.VMEM((2, *packed), jnp.float32),
            pltpu.VMEM(packed, jnp.float32),
            pltpu.VMEM((NX - 1, *packed), jnp.float32),
            pltpu.VMEM((NY - 1, *packed), jnp.float32),
            pltpu.VMEM((NZ - 1, *packed), jnp.float32),
            pltpu.VMEM((3, *packed), jnp.float32),
            pltpu.VMEM((2, *packed), jnp.float32),
            pltpu.SemaphoreType.DMA((3,)),
            pltpu.SemaphoreType.DMA((N_COPIES,)),
            pltpu.SemaphoreType.DMA((N_COPIES,)),
        ],
        compiler_params=pltpu.CompilerParams(
            collective_id=0, has_side_effects=True, vmem_limit_bytes=67043328
        ),
        name="nystrom",
    )(embeddings, sketch.T)
    return both[:RANK].T, both[RANK:].T


def solution(mesh):
    torus = Mesh(mesh.devices.reshape(NX, 2, NY, NZ), AXES)
    spec = P(AXES, None)
    return jax.shard_map(
        per_device, mesh=torus, in_specs=(spec, spec), out_specs=(spec, spec), check_vma=False
    )
```

```python
import functools
import math

import jax
import jax.numpy as jnp
from jax import lax
from jax.experimental import pallas as pl
from jax.experimental.pallas import tpu as pltpu
from jax.sharding import Mesh
from jax.sharding import PartitionSpec as P

MESH = pl.DeviceIdType.MESH
AXES = ("x", "core", "y", "z")
NX, NY, NZ = 4, 4, 8
PTS, WIDTH, RANK = 128, 512, 64
PLANE = [
    (0, 0),
    (1, 0), (3, 0), (0, 1), (0, 3),
    (1, 1), (3, 1), (1, 3), (3, 3), (2, 0), (0, 2),
    (2, 1), (2, 3), (1, 2), (3, 2),
    (2, 2),
]
LINE = [0, 1, 7, 2, 6, 3, 5, 4]
PLANE_AT = {offset: at for at, offset in enumerate(PLANE)}
LINE_AT = {offset: at for at, offset in enumerate(LINE)}
N_COPIES = 128
PART = jnp.float32


def high_dot(left, right, dims):
    return lax.dot_general(
        left, right, (dims, ((), ())),
        precision=lax.Precision.HIGHEST,
        preferred_element_type=jnp.float32,
    )


def side_by_side(block):
    half = block.shape[0] // 2
    return jnp.concatenate([block[:half], block[half:]], axis=1)


def one_above_other(block):
    half = block.shape[1] // 2
    return jnp.concatenate([block[:, :half], block[:, half:]], axis=0)


def inverses_of_cholesky(matrices):
    n = matrices[0].shape[0]
    sub = lax.broadcasted_iota(jnp.int32, (n, n), 0)
    lane = lax.broadcasted_iota(jnp.int32, (n, n), 1)
    unit = (sub == lane).astype(jnp.float32)
    tile = 8
    count = n // tile
    in_tile = lax.broadcasted_iota(jnp.int32, (tile, 2 * n), 0)
    every = range(len(matrices))
    tiles = []
    for matrix in matrices:
        work = jnp.concatenate([matrix, unit], axis=1)
        tiles.append([work[t * tile : (t + 1) * tile] for t in range(count)])
    for p in range(count):
        base = p * tile
        rows = [tiles[i][p] for i in every]
        cols = [
            [
                [jnp.broadcast_to(tiles[i][t][:, base + k : base + k + 1], (tile, 2 * n)) for t in range(p, count)]
                for k in range(tile)
            ]
            for i in every
        ]
        done = [[] for _ in every]
        for k in range(tile):
            inv = [lax.rsqrt(jnp.broadcast_to(cols[i][k][0][k : k + 1], (tile, 2 * n))) for i in every]
            low = [[c * inv[i] for c in cols[i][k]] for i in every]
            row = [jnp.broadcast_to(rows[i][k : k + 1], (tile, 2 * n)) * inv[i] for i in every]
            for m in range(k + 1, tile):
                for i in every:
                    scale = jnp.broadcast_to(low[i][0][m : m + 1], (tile, 2 * n))
                    cols[i][m] = [c - l * scale for c, l in zip(cols[i][m], low[i])]
            for i in every:
                rows[i] = jnp.where(
                    in_tile > k, rows[i] - low[i][0] * row[i], jnp.where(in_tile == k, row[i], rows[i])
                )
                done[i].append((low[i], row[i]))
        for t in range(p + 1, count):
            for i in every:
                acc = tiles[i][t]
                for low, row in done[i]:
                    acc = acc - low[t - p] * row
                tiles[i][t] = acc
        for i in every:
            tiles[i][p] = rows[i]
    return [jnp.concatenate(tiles[i], axis=0)[:, n:] for i in every]


def kernel(
    e_ref, s_ref, both_ref,
    ea, eb, sd, naf, nbf, y_acc, tests_ref, rs_out, rs_in, gram, g_part, g_x, g_y, g_z, g_sum,
    send_sem, recv_sem,
):
    me = {axis: lax.axis_index(axis) for axis in AXES}
    core = me["core"]
    coef = 3.0 / WIDTH * math.log2(math.e)

    def shift(axis, by, size):
        return lax.rem(me[axis] + by, size)

    def plane_peer(dx, dy):
        return {"x": shift("x", dx, NX), "y": shift("y", dy, NY)}

    partner = {"core": 1 - core}
    left, right = plane_peer(NX - 1, 0), plane_peer(1, 0)
    down, up = plane_peer(0, NY - 1), plane_peer(0, 1)
    below, above = {"z": shift("z", NZ - 1, NZ)}, {"z": shift("z", 1, NZ)}

    copies = {}

    def describe(key, src, dst, to):
        at = len(copies)
        assert key not in copies
        copies[key] = pltpu.make_async_remote_copy(
            src_ref=src, dst_ref=dst,
            send_sem=send_sem.at[at], recv_sem=recv_sem.at[at],
            device_id=to, device_id_type=MESH,
        )
        return copies[key]

    def send(key, src, dst, to):
        describe(key, src, dst, to).start()

    def arrived(*keys):
        for key in keys:
            copies[key].wait_recv()

    barrier = pltpu.get_barrier_semaphore()
    peers = [partner, left, right, down, up, below, above, plane_peer(2, 0), plane_peer(0, 2)]
    for peer in peers:
        pl.semaphore_signal(barrier, inc=1, device_id=peer, device_id_type=MESH)
    pl.semaphore_wait(barrier, len(peers))

    def send_plane(offset, rows, to, by):
        dx, dy = offset
        there = ((dx + by[0]) % NX, (dy + by[1]) % NY)
        lo, hi = rows
        source = e_ref if offset == (0, 0) else eb.at[pl.ds(PLANE_AT[offset] * PTS, PTS)]
        send(
            (there, lo),
            source.at[pl.ds(lo, hi - lo)],
            eb.at[pl.ds(PLANE_AT[there] * PTS + lo, hi - lo)],
            to,
        )

    def to_left(offset, lo, hi):
        send_plane(offset, (lo, hi), left, (1, 0))

    def to_right(offset, lo, hi):
        send_plane(offset, (lo, hi), right, (-1, 0))

    def to_down(offset, lo, hi):
        send_plane(offset, (lo, hi), down, (0, 1))

    def to_up(offset, lo, hi):
        send_plane(offset, (lo, hi), up, (0, -1))

    def send_line(offset, lo, hi, to, by):
        there = (offset + by) % NZ
        source = e_ref if offset == 0 else ea.at[LINE_AT[offset], pl.ds(0, PTS)]
        send(("line", there, lo), source.at[pl.ds(lo, hi - lo)], ea.at[LINE_AT[there], pl.ds(lo, hi - lo)], to)

    def send_side(offset, to, by):
        there = (offset + by) % NZ
        a, b = LINE_AT[offset], LINE_AT[there]
        send(("side", there), sd.at[a, :, pl.ds(0, PTS)], sd.at[b, :, pl.ds(0, PTS)], to)

    def send_partner(offset):
        a = LINE_AT[offset]
        source = e_ref if offset == 0 else ea.at[a, pl.ds(0, PTS)]
        send(("pline", offset), source, ea.at[a, pl.ds(PTS, PTS)], partner)

    def send_partner_side(offset):
        a = LINE_AT[offset]
        send(("pside", offset), sd.at[a, :, pl.ds(0, PTS)], sd.at[a, :, pl.ds(PTS, PTS)], partner)

    def norms_of_line(offset):
        arrived(("pside", offset), ("pline", offset))
        a = LINE_AT[offset]
        parts = sd[a, RANK : RANK + 16, :].astype(jnp.float32)
        total = (parts[0:1] + parts[1:2]) + parts[2:3]
        naf[a] = jnp.broadcast_to(total * coef, (8, 2 * PTS))

    def norms_of_plane(lo, hi):
        for at in range(lo, hi):
            block = eb[at * PTS : (at + 1) * PTS].astype(jnp.float32)
            total = jnp.sum(block * block, axis=1, keepdims=True) * coef
            nbf[at * PTS : (at + 1) * PTS] = jnp.broadcast_to(total, (PTS, 128))

    def multiply(lines, lo, hi, first=False):
        at = lo
        while at < hi:
            blocks = min(4, hi - at)
            rows = slice(at * PTS, (at + blocks) * PTS)
            total = None
            for a in lines:
                cross = lax.dot_general(
                    eb[rows], ea[a], (((1,), (1,)), ((), ())), preferred_element_type=jnp.float32
                )
                side = jnp.concatenate([nbf[rows], nbf[rows]], axis=1)
                tile = jnp.exp2(cross * (2.0 * coef) - naf[a, 0:1] - side).astype(jnp.bfloat16)
                term = lax.dot_general(
                    tile, sd[a, 0:RANK], (((1,), (1,)), ((), ())), preferred_element_type=jnp.float32
                )
                total = term if total is None else total + term
            y_acc[rows] = total if first else y_acc[rows] + total
            at += blocks

    def across(axis, lo, hi):
        there, to = ((2, 0), plane_peer(2, 0)) if axis == "x" else ((0, 2), plane_peer(0, 2))
        send_plane((0, 0), (lo, hi), to, there)

    def line_on(offset, lo, hi, to, by):
        arrived(("line", offset, lo))
        send_line(offset, lo, hi, to, by)

    def side_on(offset, to, by):
        arrived(("side", offset))
        send_side(offset, to, by)
        send_partner_side(offset)

    own = (0, 0)
    send_line(0, 0, 64, below, 1)
    send_line(0, 0, 64, above, -1)
    to_left(own, 0, 64)
    to_right(own, 0, 64)
    to_down(own, 64, 128)
    to_up(own, 64, 128)
    across("x", 0, 64)
    across("y", 64, 128)
    send_line(0, 64, 128, below, 1)
    send_line(0, 64, 128, above, -1)
    to_left(own, 64, 128)
    to_right(own, 64, 128)
    to_down(own, 0, 64)
    to_up(own, 0, 64)
    send_partner(0)
    points = e_ref[...].astype(jnp.float32)
    norms = high_dot(jnp.ones((16, WIDTH), jnp.float32), points * points, ((1,), (1,)))
    one = norms.astype(jnp.bfloat16).astype(jnp.float32)
    two = (norms - one).astype(jnp.bfloat16).astype(jnp.float32)
    three = norms - one - two
    at_row = lax.broadcasted_iota(jnp.int32, norms.shape, 0)
    split = jnp.where(at_row == 0, one, jnp.where(at_row == 1, two, three))
    sd[0, 0:RANK, 0:PTS] = s_ref[...]
    sd[0, RANK : RANK + 16, 0:PTS] = split.astype(jnp.bfloat16)
    eb[0:PTS] = e_ref[...]
    ea[0, 0:PTS] = e_ref[...]
    tests_ref[...] = s_ref[...].astype(jnp.float32).T
    send_side(0, below, 1)
    send_side(0, above, -1)
    send_partner_side(0)
    norms_of_plane(0, 1)
    norms_of_line(0)
    multiply([0], 0, 1, first=True)

    line_on(1, 0, 64, below, 1)
    line_on(7, 0, 64, above, -1)
    arrived(((1, 0), 0))
    to_down((1, 0), 0, 64)
    to_up((1, 0), 0, 64)
    arrived(((3, 0), 0))
    to_down((3, 0), 0, 64)
    to_up((3, 0), 0, 64)
    arrived(((0, 1), 64))
    to_left((0, 1), 64, 128)
    to_right((0, 1), 64, 128)
    arrived(((0, 3), 64))
    to_left((0, 3), 64, 128)
    to_right((0, 3), 64, 128)
    line_on(1, 64, 128, below, 1)
    send_partner(1)
    line_on(7, 64, 128, above, -1)
    send_partner(7)
    arrived(((2, 0), 0))
    to_down((2, 0), 0, 64)
    to_up((2, 0), 0, 64)
    arrived(((0, 2), 64))
    to_left((0, 2), 64, 128)
    to_right((0, 2), 64, 128)
    arrived(((1, 0), 64))
    to_left((1, 0), 64, 128)
    arrived(((0, 1), 0))
    to_down((0, 1), 0, 64)
    side_on(1, below, 1)
    side_on(7, above, -1)
    arrived(((3, 0), 64), ((0, 3), 0))
    norms_of_plane(1, 5)
    multiply([0], 1, 5, first=True)
    norms_of_line(1)
    norms_of_line(7)
    multiply([1, 2], 0, 5)

    line_on(2, 0, 64, below, 1)
    line_on(6, 0, 64, above, -1)
    arrived(((1, 1), 0))
    to_down((1, 1), 0, 64)
    arrived(((3, 3), 0))
    to_up((3, 3), 0, 64)
    arrived(((1, 1), 64))
    to_left((1, 1), 64, 128)
    arrived(((3, 3), 64))
    to_right((3, 3), 64, 128)
    line_on(2, 64, 128, below, 1)
    send_partner(2)
    line_on(6, 64, 128, above, -1)
    send_partner(6)
    arrived(((2, 3), 0))
    to_up((2, 3), 0, 64)
    arrived(((3, 2), 64))
    to_right((3, 2), 64, 128)
    side_on(2, below, 1)
    side_on(6, above, -1)
    arrived(((3, 1), 0), ((3, 1), 64), ((1, 3), 0), ((1, 3), 64), ((2, 0), 64), ((0, 2), 0))
    norms_of_plane(5, 11)
    multiply([0, 1, 2], 5, 11, first=True)
    norms_of_line(2)
    norms_of_line(6)
    multiply([3, 4], 0, 11)

    line_on(3, 0, 64, below, 1)
    arrived(("line", 5, 64))
    send_line(5, 64, 128, above, -1)
    arrived(("line", 3, 64), ("line", 5, 0))
    send_partner(3)
    send_partner(5)
    side_on(3, below, 1)
    arrived(("side", 5))
    send_partner_side(5)
    arrived(((2, 1), 0), ((2, 1), 64), ((2, 3), 64), ((1, 2), 0), ((1, 2), 64), ((3, 2), 0), ((2, 2), 0), ((2, 2), 64))
    norms_of_plane(11, 16)
    multiply([0, 1, 2, 3, 4], 11, 16, first=True)
    norms_of_line(3)
    norms_of_line(5)
    multiply([5, 6], 8, 16)
    arrived(("line", 4, 0), ("line", 4, 64))
    send_partner(4)
    arrived(("side", 4))
    send_partner_side(4)
    multiply([5, 6], 0, 8)

    norms_of_line(4)
    for lo in (12, 8, 4, 0):
        multiply([7], lo, lo + 4)
        for at in reversed(range(max(lo, 1), lo + 4)):
            rs_out[at] = side_by_side(y_acc[at * PTS : (at + 1) * PTS]).astype(PART)
        for at in reversed(range(max(lo, 1), lo + 4)):
            dx, dy = PLANE[at]
            there = PLANE_AT[(-dx % NX, -dy % NY)]
            send(("part", there), rs_out.at[at], rs_in.at[there], plane_peer(dx, dy))

    total = side_by_side(y_acc[0:PTS])
    for at in range(1, 16):
        arrived(("part", at))
        total = total + rs_in[at].astype(jnp.float32)
    sketched = one_above_other(total)
    tests = tests_ref[...]
    products = high_dot(
        jnp.concatenate([tests, sketched], axis=1),
        jnp.concatenate([sketched, tests], axis=1),
        ((0,), (0,)),
    )
    top, bottom = products[:RANK], products[RANK:]
    turned = jnp.concatenate([top[:, RANK:], top[:, :RANK]], axis=1)
    lane = lax.broadcasted_iota(jnp.int32, bottom.shape, 1)
    gram[...] = jnp.where(lane < RANK, bottom, 0.5 * (bottom + turned))

    for copy in copies.values():
        copy.wait_send()
    over = describe("over", gram, g_part, partner)
    back = describe("back", g_sum.at[3], g_sum.at[3], partner)
    stages = []
    for stage, axis, size, landing in ((0, "x", NX, g_x), (1, "y", NY, g_y), (2, "z", NZ, g_z)):
        stages.append((stage, landing, [
            describe((axis, by), g_sum.at[stage], landing.at[by - 1], {axis: shift(axis, by, size)})
            for by in range(1, size)
        ]))

    @pl.when(core == 0)
    def _():
        over.start()
        over.wait_send()
        back.wait_recv()

    @pl.when(core == 1)
    def _():
        over.wait_recv()
        g_sum[0] = gram[...] + g_part[...]
        for stage, landing, group in stages:
            for copy in group:
                copy.start()
            value = g_sum[stage]
            for at, copy in enumerate(group):
                copy.wait_recv()
                value = value + landing[at]
            g_sum[stage + 1] = value
        back.start()
        for _, _, group in stages:
            for copy in group:
                copy.wait_send()
        back.wait_send()

    both = g_sum[3]
    low = jnp.concatenate(inverses_of_cholesky([both[:, :RANK], both[:, RANK:]]), axis=0)
    both_ref[...] = high_dot(low, sketched, ((1,), (1,))) * math.sqrt(PTS * 256)
    assert len(copies) <= N_COPIES


def per_device(embeddings, sketch):
    vmem = pl.BlockSpec(memory_space=pltpu.VMEM)
    pair = (RANK, 2 * RANK)
    both = pl.pallas_call(
        kernel,
        out_shape=jax.ShapeDtypeStruct((2 * RANK, PTS), jnp.float32),
        in_specs=[vmem, vmem],
        out_specs=vmem,
        scratch_shapes=[
            pltpu.VMEM((NZ, 2 * PTS, WIDTH), jnp.bfloat16),
            pltpu.VMEM((16 * PTS, WIDTH), jnp.bfloat16),
            pltpu.VMEM((NZ, RANK + 16, 2 * PTS), jnp.bfloat16),
            pltpu.VMEM((NZ, 8, 2 * PTS), jnp.float32),
            pltpu.VMEM((16 * PTS, 128), jnp.float32),
            pltpu.VMEM((16 * PTS, RANK), jnp.float32),
            pltpu.VMEM((PTS, RANK), jnp.float32),
            pltpu.VMEM((16, PTS // 2, 2 * RANK), PART),
            pltpu.VMEM((16, PTS // 2, 2 * RANK), PART),
            pltpu.VMEM(pair, jnp.float32),
            pltpu.VMEM(pair, jnp.float32),
            pltpu.VMEM((NX - 1, *pair), jnp.float32),
            pltpu.VMEM((NY - 1, *pair), jnp.float32),
            pltpu.VMEM((NZ - 1, *pair), jnp.float32),
            pltpu.VMEM((4, *pair), jnp.float32),
            pltpu.SemaphoreType.DMA((N_COPIES,)),
            pltpu.SemaphoreType.DMA((N_COPIES,)),
        ],
        compiler_params=pltpu.CompilerParams(
            collective_id=0, has_side_effects=True, vmem_limit_bytes=24 << 20
        ),
        name="nystrom",
    )(embeddings, sketch.T)
    return both[:RANK].T, both[RANK:].T


def solution(mesh):
    torus = Mesh(mesh.devices.reshape(NX, 2, NY, NZ), AXES)
    spec = P(AXES, None)
    return jax.shard_map(
        per_device, mesh=torus, in_specs=(spec, spec), out_specs=(spec, spec), check_vma=False
    )
```

```python
import functools
import math

import jax
import jax.numpy as jnp
from jax import lax
from jax.experimental import pallas as pl
from jax.experimental.pallas import tpu as pltpu
from jax.sharding import Mesh
from jax.sharding import PartitionSpec as P

MESH = pl.DeviceIdType.MESH
AXES = ("x", "core", "y", "z")
NX, NY, NZ = 4, 4, 8
PTS, WIDTH, RANK = 128, 512, 64
PLANE = [
    (0, 0),
    (1, 0), (3, 0), (0, 1), (0, 3),
    (1, 1), (3, 1), (1, 3), (3, 3), (2, 0), (0, 2),
    (2, 1), (2, 3), (1, 2), (3, 2),
    (2, 2),
]
LINE = [0, 1, 7, 2, 6, 3, 5, 4]
PLANE_AT = {offset: at for at, offset in enumerate(PLANE)}
LINE_AT = {offset: at for at, offset in enumerate(LINE)}
N_COPIES = 144


def high_dot(left, right, dims):
    return lax.dot_general(
        left, right, (dims, ((), ())),
        precision=lax.Precision.HIGHEST,
        preferred_element_type=jnp.float32,
    )


def side_by_side(block):
    half = block.shape[0] // 2
    return jnp.concatenate([block[:half], block[half:]], axis=1)


def one_above_other(block):
    half = block.shape[1] // 2
    return jnp.concatenate([block[:, :half], block[:, half:]], axis=0)


def inverses_of_cholesky(matrices):
    n = matrices[0].shape[0]
    sub = lax.broadcasted_iota(jnp.int32, (n, n), 0)
    lane = lax.broadcasted_iota(jnp.int32, (n, n), 1)
    unit = (sub == lane).astype(jnp.float32)
    tile = 8
    count = n // tile
    in_tile = lax.broadcasted_iota(jnp.int32, (tile, 2 * n), 0)
    every = range(len(matrices))
    tiles = []
    for matrix in matrices:
        work = jnp.concatenate([matrix, unit], axis=1)
        tiles.append([work[t * tile : (t + 1) * tile] for t in range(count)])
    for p in range(count):
        base = p * tile
        rows = [tiles[i][p] for i in every]
        cols = [
            [
                [jnp.broadcast_to(tiles[i][t][:, base + k : base + k + 1], (tile, 2 * n)) for t in range(p, count)]
                for k in range(tile)
            ]
            for i in every
        ]
        done = [[] for _ in every]
        for k in range(tile):
            inv = [lax.rsqrt(jnp.broadcast_to(cols[i][k][0][k : k + 1], (tile, 2 * n))) for i in every]
            low = [[c * inv[i] for c in cols[i][k]] for i in every]
            row = [jnp.broadcast_to(rows[i][k : k + 1], (tile, 2 * n)) * inv[i] for i in every]
            for m in range(k + 1, tile):
                for i in every:
                    scale = jnp.broadcast_to(low[i][0][m : m + 1], (tile, 2 * n))
                    cols[i][m] = [c - l * scale for c, l in zip(cols[i][m], low[i])]
            for i in every:
                rows[i] = jnp.where(
                    in_tile > k, rows[i] - low[i][0] * row[i], jnp.where(in_tile == k, row[i], rows[i])
                )
                done[i].append((low[i], row[i]))
        for t in range(p + 1, count):
            for i in every:
                acc = tiles[i][t]
                for low, row in done[i]:
                    acc = acc - low[t - p] * row
                tiles[i][t] = acc
        for i in every:
            tiles[i][p] = rows[i]
    return [jnp.concatenate(tiles[i], axis=0)[:, n:] for i in every]


def kernel(
    e_ref, s_ref, both_ref,
    ea, eb, sd, naf, nbf, y_acc, tests_ref, rs_out, rs_in, owned, g_x, g_y, g_z, g_sum,
    send_sem, recv_sem,
):
    me = {axis: lax.axis_index(axis) for axis in AXES}
    core = me["core"]
    coef = 3.0 / WIDTH * math.log2(math.e)

    def shift(axis, by, size):
        return lax.rem(me[axis] + by, size)

    def plane_peer(dx, dy):
        return {"x": shift("x", dx, NX), "y": shift("y", dy, NY)}

    partner = {"core": 1 - core}
    left, right = plane_peer(NX - 1, 0), plane_peer(1, 0)
    down, up = plane_peer(0, NY - 1), plane_peer(0, 1)
    below, above = {"z": shift("z", NZ - 1, NZ)}, {"z": shift("z", 1, NZ)}

    copies = {}

    def describe(key, src, dst, to):
        at = len(copies)
        assert key not in copies
        copies[key] = pltpu.make_async_remote_copy(
            src_ref=src, dst_ref=dst,
            send_sem=send_sem.at[at], recv_sem=recv_sem.at[at],
            device_id=to, device_id_type=MESH,
        )
        return copies[key]

    def send(key, src, dst, to):
        describe(key, src, dst, to).start()

    def arrived(*keys):
        for key in keys:
            copies[key].wait_recv()

    barrier = pltpu.get_barrier_semaphore()
    peers = [partner, left, right, down, up, below, above, plane_peer(2, 0), plane_peer(0, 2)]
    for peer in peers:
        pl.semaphore_signal(barrier, inc=1, device_id=peer, device_id_type=MESH)
    pl.semaphore_wait(barrier, len(peers))

    def send_plane(offset, rows, to, by):
        dx, dy = offset
        there = ((dx + by[0]) % NX, (dy + by[1]) % NY)
        lo, hi = rows
        source = e_ref if offset == (0, 0) else eb.at[pl.ds(PLANE_AT[offset] * PTS, PTS)]
        send(
            (there, lo),
            source.at[pl.ds(lo, hi - lo)],
            eb.at[pl.ds(PLANE_AT[there] * PTS + lo, hi - lo)],
            to,
        )

    def to_left(offset, lo, hi):
        send_plane(offset, (lo, hi), left, (1, 0))

    def to_right(offset, lo, hi):
        send_plane(offset, (lo, hi), right, (-1, 0))

    def to_down(offset, lo, hi):
        send_plane(offset, (lo, hi), down, (0, 1))

    def to_up(offset, lo, hi):
        send_plane(offset, (lo, hi), up, (0, -1))

    def send_line(offset, lo, hi, to, by):
        there = (offset + by) % NZ
        source = e_ref if offset == 0 else ea.at[LINE_AT[offset], pl.ds(0, PTS)]
        send(("line", there, lo), source.at[pl.ds(lo, hi - lo)], ea.at[LINE_AT[there], pl.ds(lo, hi - lo)], to)

    def send_side(offset, to, by):
        there = (offset + by) % NZ
        a, b = LINE_AT[offset], LINE_AT[there]
        send(("side", there), sd.at[a, :, pl.ds(0, PTS)], sd.at[b, :, pl.ds(0, PTS)], to)

    def send_partner(offset):
        a = LINE_AT[offset]
        source = e_ref if offset == 0 else ea.at[a, pl.ds(0, PTS)]
        send(("pline", offset), source, ea.at[a, pl.ds(PTS, PTS)], partner)

    def send_partner_side(offset):
        a = LINE_AT[offset]
        send(("pside", offset), sd.at[a, :, pl.ds(0, PTS)], sd.at[a, :, pl.ds(PTS, PTS)], partner)

    def norms_of_line(offset):
        arrived(("pside", offset), ("pline", offset))
        a = LINE_AT[offset]
        parts = sd[a, RANK : RANK + 16, :].astype(jnp.float32)
        total = (parts[0:1] + parts[1:2]) + parts[2:3]
        naf[a] = jnp.broadcast_to(total * coef, (8, 2 * PTS))

    def norms_of_plane(lo, hi):
        for at in range(lo, hi):
            block = eb[at * PTS : (at + 1) * PTS].astype(jnp.float32)
            total = jnp.sum(block * block, axis=1, keepdims=True) * coef
            nbf[at * PTS : (at + 1) * PTS] = jnp.broadcast_to(total, (PTS, 128))

    def multiply(lines, lo, hi, first=False):
        at = lo
        while at < hi:
            blocks = min(4, hi - at)
            rows = slice(at * PTS, (at + blocks) * PTS)
            total = None
            for a in lines:
                cross = lax.dot_general(
                    eb[rows], ea[a], (((1,), (1,)), ((), ())), preferred_element_type=jnp.float32
                )
                side = jnp.concatenate([nbf[rows], nbf[rows]], axis=1)
                tile = jnp.exp2(cross * (2.0 * coef) - naf[a, 0:1] - side).astype(jnp.bfloat16)
                term = lax.dot_general(
                    tile, sd[a, 0:RANK], (((1,), (1,)), ((), ())), preferred_element_type=jnp.float32
                )
                total = term if total is None else total + term
            y_acc[rows] = total if first else y_acc[rows] + total
            at += blocks

    def across(axis, lo, hi):
        there, to = ((2, 0), plane_peer(2, 0)) if axis == "x" else ((0, 2), plane_peer(0, 2))
        send_plane((0, 0), (lo, hi), to, there)

    def line_on(offset, lo, hi, to, by):
        arrived(("line", offset, lo))
        send_line(offset, lo, hi, to, by)

    def side_on(offset, to, by):
        arrived(("side", offset))
        send_side(offset, to, by)
        send_partner_side(offset)

    own = (0, 0)
    send_line(0, 0, 64, below, 1)
    send_line(0, 0, 64, above, -1)
    to_left(own, 0, 64)
    to_right(own, 0, 64)
    to_down(own, 64, 128)
    to_up(own, 64, 128)
    across("x", 0, 64)
    across("y", 64, 128)
    send_line(0, 64, 128, below, 1)
    send_line(0, 64, 128, above, -1)
    to_left(own, 64, 128)
    to_right(own, 64, 128)
    to_down(own, 0, 64)
    to_up(own, 0, 64)
    send_partner(0)
    points = e_ref[...].astype(jnp.float32)
    norms = high_dot(jnp.ones((16, WIDTH), jnp.float32), points * points, ((1,), (1,)))
    one = norms.astype(jnp.bfloat16).astype(jnp.float32)
    two = (norms - one).astype(jnp.bfloat16).astype(jnp.float32)
    three = norms - one - two
    at_row = lax.broadcasted_iota(jnp.int32, norms.shape, 0)
    split = jnp.where(at_row == 0, one, jnp.where(at_row == 1, two, three))
    sd[0, 0:RANK, 0:PTS] = s_ref[...]
    sd[0, RANK : RANK + 16, 0:PTS] = split.astype(jnp.bfloat16)
    eb[0:PTS] = e_ref[...]
    ea[0, 0:PTS] = e_ref[...]
    tests_ref[0] = s_ref[...].astype(jnp.float32).T
    send_side(0, below, 1)
    send_side(0, above, -1)
    send_partner_side(0)
    norms_of_plane(0, 1)
    norms_of_line(0)
    tests_ref[1] = sd[0, 0:RANK, PTS : 2 * PTS].astype(jnp.float32).T
    multiply([0], 0, 1, first=True)

    line_on(1, 0, 64, below, 1)
    line_on(7, 0, 64, above, -1)
    arrived(((1, 0), 0))
    to_down((1, 0), 0, 64)
    to_up((1, 0), 0, 64)
    arrived(((3, 0), 0))
    to_down((3, 0), 0, 64)
    to_up((3, 0), 0, 64)
    arrived(((0, 1), 64))
    to_left((0, 1), 64, 128)
    to_right((0, 1), 64, 128)
    arrived(((0, 3), 64))
    to_left((0, 3), 64, 128)
    to_right((0, 3), 64, 128)
    line_on(1, 64, 128, below, 1)
    send_partner(1)
    line_on(7, 64, 128, above, -1)
    send_partner(7)
    arrived(((2, 0), 0))
    to_down((2, 0), 0, 64)
    to_up((2, 0), 0, 64)
    arrived(((0, 2), 64))
    to_left((0, 2), 64, 128)
    to_right((0, 2), 64, 128)
    arrived(((1, 0), 64))
    to_left((1, 0), 64, 128)
    arrived(((0, 1), 0))
    to_down((0, 1), 0, 64)
    side_on(1, below, 1)
    side_on(7, above, -1)
    arrived(((3, 0), 64), ((0, 3), 0))
    norms_of_plane(1, 5)
    multiply([0], 1, 5, first=True)
    norms_of_line(1)
    norms_of_line(7)
    multiply([1, 2], 0, 5)

    line_on(2, 0, 64, below, 1)
    line_on(6, 0, 64, above, -1)
    arrived(((1, 1), 0))
    to_down((1, 1), 0, 64)
    arrived(((3, 3), 0))
    to_up((3, 3), 0, 64)
    arrived(((1, 1), 64))
    to_left((1, 1), 64, 128)
    arrived(((3, 3), 64))
    to_right((3, 3), 64, 128)
    line_on(2, 64, 128, below, 1)
    send_partner(2)
    line_on(6, 64, 128, above, -1)
    send_partner(6)
    arrived(((2, 3), 0))
    to_up((2, 3), 0, 64)
    arrived(((3, 2), 64))
    to_right((3, 2), 64, 128)
    side_on(2, below, 1)
    side_on(6, above, -1)
    arrived(((3, 1), 0), ((3, 1), 64), ((1, 3), 0), ((1, 3), 64), ((2, 0), 64), ((0, 2), 0))
    norms_of_plane(5, 11)
    multiply([0, 1, 2], 5, 11, first=True)
    norms_of_line(2)
    norms_of_line(6)
    multiply([3, 4], 0, 11)

    line_on(3, 0, 64, below, 1)
    arrived(("line", 5, 64))
    send_line(5, 64, 128, above, -1)
    arrived(("line", 3, 64), ("line", 5, 0))
    send_partner(3)
    send_partner(5)
    side_on(3, below, 1)
    arrived(("side", 5))
    send_partner_side(5)
    arrived(((2, 1), 0), ((2, 1), 64), ((2, 3), 64), ((1, 2), 0), ((1, 2), 64), ((3, 2), 0), ((2, 2), 0), ((2, 2), 64))
    norms_of_plane(11, 16)
    multiply([0, 1, 2, 3, 4], 11, 16, first=True)
    norms_of_line(3)
    norms_of_line(5)
    multiply([5, 6], 8, 16)
    arrived(("line", 4, 0), ("line", 4, 64))
    send_partner(4)
    arrived(("side", 4))
    send_partner_side(4)
    multiply([5, 6], 0, 8)

    gathers = list(copies.values())
    norms_of_line(4)
    for lo in (12, 8, 4, 0):
        multiply([7], lo, lo + 4)
        for at in reversed(range(lo, lo + 4)):
            rs_out[at] = side_by_side(y_acc[at * PTS : (at + 1) * PTS])
        group = []
        for at in reversed(range(lo, lo + 4)):
            dx, dy = PLANE[at]
            there = PLANE_AT[(-dx % NX, -dy % NY)]
            for c in range(2):
                to = partner if at == 0 else {**plane_peer(dx, dy), "core": 1}
                if at > 0 or c == 0:
                    group.append((c, describe(("part", c, there), rs_out.at[at], rs_in.at[c, there], to)))
        for c in range(2):

            @pl.when(core == c)
            def _():
                for whose, copy in group:
                    if whose == c:
                        copy.start()

    to_partner = describe("rows", owned.at[0], owned.at[0], partner)
    back = describe("back", g_sum.at[3], g_sum.at[3], partner)
    stages = []
    for stage, axis, size, landing in ((0, "x", NX, g_x), (1, "y", NY, g_y), (2, "z", NZ, g_z)):
        stages.append((stage, landing, [
            describe((axis, by), g_sum.at[stage], landing.at[by - 1], {axis: shift(axis, by, size)})
            for by in range(1, size)
        ]))

    def given(c):
        return [copies[("part", c, at)] for at in range(1 if c else 0, 16)]

    @pl.when(core == 0)
    def _():
        for copy in given(0):
            copy.wait_send()
        to_partner.wait_recv()
        back.wait_recv()

    @pl.when(core == 1)
    def _():
        totals = []
        for c in range(2):
            total = None if c == 0 else rs_out[0]
            for at in range(1 if c else 0, 16):
                copies[("part", c, at)].wait_recv()
                term = rs_in[c, at]
                total = term if total is None else total + term
            totals.append(total)
            owned[c] = total
            if c == 0:
                to_partner.start()
        sketched = jnp.concatenate([one_above_other(total) for total in totals], axis=0)
        tests = jnp.concatenate([tests_ref[1], tests_ref[0]], axis=0)
        products = high_dot(
            jnp.concatenate([tests, sketched], axis=1),
            jnp.concatenate([sketched, tests], axis=1),
            ((0,), (0,)),
        )
        top, bottom = products[:RANK], products[RANK:]
        turned = jnp.concatenate([top[:, RANK:], top[:, :RANK]], axis=1)
        lane = lax.broadcasted_iota(jnp.int32, bottom.shape, 1)
        g_sum[0] = jnp.where(lane < RANK, bottom, 0.5 * (bottom + turned))
        for stage, landing, group in stages:
            for copy in group:
                copy.start()
            value = g_sum[stage]
            for at, copy in enumerate(group):
                copy.wait_recv()
                value = value + landing[at]
            g_sum[stage + 1] = value
        back.start()
        for _, _, group in stages:
            for copy in group:
                copy.wait_send()
        for copy in given(1):
            copy.wait_send()
        to_partner.wait_send()
        back.wait_send()

    for copy in gathers:
        copy.wait_send()
    sketched = one_above_other(owned[core])
    both = g_sum[3]
    low = jnp.concatenate(inverses_of_cholesky([both[:, :RANK], both[:, RANK:]]), axis=0)
    both_ref[...] = high_dot(low, sketched, ((1,), (1,))) * math.sqrt(PTS * 256)
    assert len(copies) <= N_COPIES


def per_device(embeddings, sketch):
    vmem = pl.BlockSpec(memory_space=pltpu.VMEM)
    pair = (RANK, 2 * RANK)
    both = pl.pallas_call(
        kernel,
        out_shape=jax.ShapeDtypeStruct((2 * RANK, PTS), jnp.float32),
        in_specs=[vmem, vmem],
        out_specs=vmem,
        scratch_shapes=[
            pltpu.VMEM((NZ, 2 * PTS, WIDTH), jnp.bfloat16),
            pltpu.VMEM((16 * PTS, WIDTH), jnp.bfloat16),
            pltpu.VMEM((NZ, RANK + 16, 2 * PTS), jnp.bfloat16),
            pltpu.VMEM((NZ, 8, 2 * PTS), jnp.float32),
            pltpu.VMEM((16 * PTS, 128), jnp.float32),
            pltpu.VMEM((16 * PTS, RANK), jnp.float32),
            pltpu.VMEM((2, PTS, RANK), jnp.float32),
            pltpu.VMEM((16, PTS // 2, 2 * RANK), jnp.float32),
            pltpu.VMEM((2, 16, PTS // 2, 2 * RANK), jnp.float32),
            pltpu.VMEM((2, PTS // 2, 2 * RANK), jnp.float32),
            pltpu.VMEM((NX - 1, *pair), jnp.float32),
            pltpu.VMEM((NY - 1, *pair), jnp.float32),
            pltpu.VMEM((NZ - 1, *pair), jnp.float32),
            pltpu.VMEM((4, *pair), jnp.float32),
            pltpu.SemaphoreType.DMA((N_COPIES,)),
            pltpu.SemaphoreType.DMA((N_COPIES,)),
        ],
        compiler_params=pltpu.CompilerParams(
            collective_id=0, has_side_effects=True, vmem_limit_bytes=24 << 20
        ),
        name="nystrom",
    )(embeddings, sketch.T)
    return both[:RANK].T, both[RANK:].T


def solution(mesh):
    torus = Mesh(mesh.devices.reshape(NX, 2, NY, NZ), AXES)
    spec = P(AXES, None)
    return jax.shard_map(
        per_device, mesh=torus, in_specs=(spec, spec), out_specs=(spec, spec), check_vma=False
    )
```

```python
import functools
import math

import jax
import jax.numpy as jnp
from jax import lax
from jax.experimental import pallas as pl
from jax.experimental.pallas import tpu as pltpu
from jax.sharding import Mesh
from jax.sharding import PartitionSpec as P

MESH = pl.DeviceIdType.MESH
AXES = ("x", "core", "y", "z")
NX, NY, NZ = 4, 4, 8
PTS, WIDTH, RANK = 128, 512, 64
PLANE = [
    (0, 0),
    (1, 0), (3, 0), (0, 1), (0, 3),
    (1, 1), (3, 1), (1, 3), (3, 3), (2, 0), (0, 2),
    (2, 1), (2, 3), (1, 2), (3, 2),
    (2, 2),
]
LINE = [0, 1, 7, 2, 6, 3, 5, 4]
PLANE_AT = {offset: at for at, offset in enumerate(PLANE)}
LINE_AT = {offset: at for at, offset in enumerate(LINE)}
N_COPIES = 144


def high_dot(left, right, dims):
    return lax.dot_general(
        left, right, (dims, ((), ())),
        precision=lax.Precision.HIGHEST,
        preferred_element_type=jnp.float32,
    )


def side_by_side(block):
    half = block.shape[0] // 2
    return jnp.concatenate([block[:half], block[half:]], axis=1)


def one_above_other(block):
    half = block.shape[1] // 2
    return jnp.concatenate([block[:, :half], block[:, half:]], axis=0)


def inverses_of_cholesky(matrices):
    n = matrices[0].shape[0]
    sub = lax.broadcasted_iota(jnp.int32, (n, n), 0)
    lane = lax.broadcasted_iota(jnp.int32, (n, n), 1)
    unit = (sub == lane).astype(jnp.float32)
    tile = 8
    count = n // tile
    in_tile = lax.broadcasted_iota(jnp.int32, (tile, 2 * n), 0)
    every = range(len(matrices))
    tiles = []
    for matrix in matrices:
        work = jnp.concatenate([matrix, unit], axis=1)
        tiles.append([work[t * tile : (t + 1) * tile] for t in range(count)])
    for p in range(count):
        base = p * tile
        rows = [tiles[i][p] for i in every]
        cols = [
            [
                [jnp.broadcast_to(tiles[i][t][:, base + k : base + k + 1], (tile, 2 * n)) for t in range(p, count)]
                for k in range(tile)
            ]
            for i in every
        ]
        done = [[] for _ in every]
        for k in range(tile):
            inv = [lax.rsqrt(jnp.broadcast_to(cols[i][k][0][k : k + 1], (tile, 2 * n))) for i in every]
            low = [[c * inv[i] for c in cols[i][k]] for i in every]
            row = [jnp.broadcast_to(rows[i][k : k + 1], (tile, 2 * n)) * inv[i] for i in every]
            for m in range(k + 1, tile):
                for i in every:
                    scale = jnp.broadcast_to(low[i][0][m : m + 1], (tile, 2 * n))
                    cols[i][m] = [c - l * scale for c, l in zip(cols[i][m], low[i])]
            for i in every:
                rows[i] = jnp.where(
                    in_tile > k, rows[i] - low[i][0] * row[i], jnp.where(in_tile == k, row[i], rows[i])
                )
                done[i].append((low[i], row[i]))
        for t in range(p + 1, count):
            for i in every:
                acc = tiles[i][t]
                for low, row in done[i]:
                    acc = acc - low[t - p] * row
                tiles[i][t] = acc
        for i in every:
            tiles[i][p] = rows[i]
    return [jnp.concatenate(tiles[i], axis=0)[:, n:] for i in every]


def kernel(
    e_ref, s_ref, both_ref,
    ea, eb, sd, naf, nbf, y_acc, tests_ref, rs_out, rs_in, owned, g_x, g_y, g_z, g_sum,
    send_sem, recv_sem,
):
    me = {axis: lax.axis_index(axis) for axis in AXES}
    core = me["core"]
    coef = 3.0 / WIDTH * math.log2(math.e)

    def shift(axis, by, size):
        return lax.rem(me[axis] + by, size)

    def plane_peer(dx, dy):
        return {"x": shift("x", dx, NX), "y": shift("y", dy, NY)}

    partner = {"core": 1 - core}
    left, right = plane_peer(NX - 1, 0), plane_peer(1, 0)
    down, up = plane_peer(0, NY - 1), plane_peer(0, 1)
    below, above = {"z": shift("z", NZ - 1, NZ)}, {"z": shift("z", 1, NZ)}

    copies = {}

    def describe(key, src, dst, to):
        at = len(copies)
        assert key not in copies
        copies[key] = pltpu.make_async_remote_copy(
            src_ref=src, dst_ref=dst,
            send_sem=send_sem.at[at], recv_sem=recv_sem.at[at],
            device_id=to, device_id_type=MESH,
        )
        return copies[key]

    def send(key, src, dst, to):
        describe(key, src, dst, to).start()

    def arrived(*keys):
        for key in keys:
            copies[key].wait_recv()

    barrier = pltpu.get_barrier_semaphore()
    peers = [partner, left, right, down, up, below, above, plane_peer(2, 0), plane_peer(0, 2)]
    for peer in peers:
        pl.semaphore_signal(barrier, inc=1, device_id=peer, device_id_type=MESH)
    pl.semaphore_wait(barrier, len(peers))

    def send_plane(offset, rows, to, by):
        dx, dy = offset
        there = ((dx + by[0]) % NX, (dy + by[1]) % NY)
        lo, hi = rows
        source = e_ref if offset == (0, 0) else eb.at[pl.ds(PLANE_AT[offset] * PTS, PTS)]
        send(
            (there, lo),
            source.at[pl.ds(lo, hi - lo)],
            eb.at[pl.ds(PLANE_AT[there] * PTS + lo, hi - lo)],
            to,
        )

    def to_left(offset, lo, hi):
        send_plane(offset, (lo, hi), left, (1, 0))

    def to_right(offset, lo, hi):
        send_plane(offset, (lo, hi), right, (-1, 0))

    def to_down(offset, lo, hi):
        send_plane(offset, (lo, hi), down, (0, 1))

    def to_up(offset, lo, hi):
        send_plane(offset, (lo, hi), up, (0, -1))

    def send_line(offset, lo, hi, to, by):
        there = (offset + by) % NZ
        source = e_ref if offset == 0 else ea.at[LINE_AT[offset], pl.ds(0, PTS)]
        send(("line", there, lo), source.at[pl.ds(lo, hi - lo)], ea.at[LINE_AT[there], pl.ds(lo, hi - lo)], to)

    def send_side(offset, to, by):
        there = (offset + by) % NZ
        a, b = LINE_AT[offset], LINE_AT[there]
        send(("side", there), sd.at[a, :, pl.ds(0, PTS)], sd.at[b, :, pl.ds(0, PTS)], to)

    def send_partner(offset):
        a = LINE_AT[offset]
        source = e_ref if offset == 0 else ea.at[a, pl.ds(0, PTS)]
        send(("pline", offset), source, ea.at[a, pl.ds(PTS, PTS)], partner)

    def send_partner_side(offset):
        a = LINE_AT[offset]
        send(("pside", offset), sd.at[a, :, pl.ds(0, PTS)], sd.at[a, :, pl.ds(PTS, PTS)], partner)

    def norms_of_line(offset):
        arrived(("pside", offset), ("pline", offset))
        a = LINE_AT[offset]
        parts = sd[a, RANK : RANK + 16, :].astype(jnp.float32)
        total = (parts[0:1] + parts[1:2]) + parts[2:3]
        naf[a] = jnp.broadcast_to(total * coef, (8, 2 * PTS))

    def norms_of_plane(lo, hi):
        for at in range(lo, hi):
            block = eb[at * PTS : (at + 1) * PTS].astype(jnp.float32)
            total = jnp.sum(block * block, axis=1, keepdims=True) * coef
            nbf[at * PTS : (at + 1) * PTS] = jnp.broadcast_to(total, (PTS, 128))

    def multiply(lines, lo, hi, first=False):
        at = lo
        while at < hi:
            blocks = min(4, hi - at)
            rows = slice(at * PTS, (at + blocks) * PTS)
            total = None
            for a in lines:
                cross = lax.dot_general(
                    eb[rows], ea[a], (((1,), (1,)), ((), ())), preferred_element_type=jnp.float32
                )
                side = jnp.concatenate([nbf[rows], nbf[rows]], axis=1)
                tile = jnp.exp2(cross * (2.0 * coef) - naf[a, 0:1] - side).astype(jnp.bfloat16)
                term = lax.dot_general(
                    tile, sd[a, 0:RANK], (((1,), (1,)), ((), ())), preferred_element_type=jnp.float32
                )
                total = term if total is None else total + term
            y_acc[rows] = total if first else y_acc[rows] + total
            at += blocks

    def across(axis, lo, hi):
        there, to = ((2, 0), plane_peer(2, 0)) if axis == "x" else ((0, 2), plane_peer(0, 2))
        send_plane((0, 0), (lo, hi), to, there)

    def line_on(offset, lo, hi, to, by):
        arrived(("line", offset, lo))
        send_line(offset, lo, hi, to, by)

    def side_on(offset, to, by):
        arrived(("side", offset))
        send_side(offset, to, by)
        send_partner_side(offset)

    own = (0, 0)
    send_line(0, 0, 64, below, 1)
    send_line(0, 0, 64, above, -1)
    to_left(own, 0, 64)
    to_right(own, 0, 64)
    to_down(own, 64, 128)
    to_up(own, 64, 128)
    across("x", 0, 64)
    across("y", 64, 128)
    send_line(0, 64, 128, below, 1)
    send_line(0, 64, 128, above, -1)
    to_left(own, 64, 128)
    to_right(own, 64, 128)
    to_down(own, 0, 64)
    to_up(own, 0, 64)
    send_partner(0)
    points = e_ref[...].astype(jnp.float32)
    norms = high_dot(jnp.ones((16, WIDTH), jnp.float32), points * points, ((1,), (1,)))
    one = norms.astype(jnp.bfloat16).astype(jnp.float32)
    two = (norms - one).astype(jnp.bfloat16).astype(jnp.float32)
    three = norms - one - two
    at_row = lax.broadcasted_iota(jnp.int32, norms.shape, 0)
    split = jnp.where(at_row == 0, one, jnp.where(at_row == 1, two, three))
    sd[0, 0:RANK, 0:PTS] = s_ref[...]
    sd[0, RANK : RANK + 16, 0:PTS] = split.astype(jnp.bfloat16)
    eb[0:PTS] = e_ref[...]
    ea[0, 0:PTS] = e_ref[...]
    tests_ref[0] = s_ref[...].astype(jnp.float32).T
    send_side(0, below, 1)
    send_side(0, above, -1)
    send_partner_side(0)
    norms_of_plane(0, 1)
    norms_of_line(0)
    tests_ref[1] = sd[0, 0:RANK, PTS : 2 * PTS].astype(jnp.float32).T
    multiply([0], 0, 1, first=True)

    line_on(1, 0, 64, below, 1)
    line_on(7, 0, 64, above, -1)
    arrived(((1, 0), 0))
    to_down((1, 0), 0, 64)
    to_up((1, 0), 0, 64)
    arrived(((3, 0), 0))
    to_down((3, 0), 0, 64)
    to_up((3, 0), 0, 64)
    arrived(((0, 1), 64))
    to_left((0, 1), 64, 128)
    to_right((0, 1), 64, 128)
    arrived(((0, 3), 64))
    to_left((0, 3), 64, 128)
    to_right((0, 3), 64, 128)
    line_on(1, 64, 128, below, 1)
    send_partner(1)
    line_on(7, 64, 128, above, -1)
    send_partner(7)
    arrived(((2, 0), 0))
    to_down((2, 0), 0, 64)
    to_up((2, 0), 0, 64)
    arrived(((0, 2), 64))
    to_left((0, 2), 64, 128)
    to_right((0, 2), 64, 128)
    arrived(((1, 0), 64))
    to_left((1, 0), 64, 128)
    arrived(((0, 1), 0))
    to_down((0, 1), 0, 64)
    side_on(1, below, 1)
    side_on(7, above, -1)
    arrived(((3, 0), 64), ((0, 3), 0))
    norms_of_plane(1, 5)
    multiply([0], 1, 5, first=True)
    norms_of_line(1)
    norms_of_line(7)
    multiply([1, 2], 0, 5)

    line_on(2, 0, 64, below, 1)
    line_on(6, 0, 64, above, -1)
    arrived(((1, 1), 0))
    to_down((1, 1), 0, 64)
    arrived(((3, 3), 0))
    to_up((3, 3), 0, 64)
    arrived(((1, 1), 64))
    to_left((1, 1), 64, 128)
    arrived(((3, 3), 64))
    to_right((3, 3), 64, 128)
    line_on(2, 64, 128, below, 1)
    send_partner(2)
    line_on(6, 64, 128, above, -1)
    send_partner(6)
    arrived(((2, 3), 0))
    to_up((2, 3), 0, 64)
    arrived(((3, 2), 64))
    to_right((3, 2), 64, 128)
    side_on(2, below, 1)
    side_on(6, above, -1)
    arrived(((3, 1), 0), ((3, 1), 64), ((1, 3), 0), ((1, 3), 64), ((2, 0), 64), ((0, 2), 0))
    norms_of_plane(5, 11)
    multiply([0, 1, 2], 5, 11, first=True)
    norms_of_line(2)
    norms_of_line(6)
    multiply([3, 4], 0, 11)

    line_on(3, 0, 64, below, 1)
    arrived(("line", 5, 64))
    send_line(5, 64, 128, above, -1)
    arrived(("line", 3, 64), ("line", 5, 0))
    send_partner(3)
    send_partner(5)
    side_on(3, below, 1)
    arrived(("side", 5))
    send_partner_side(5)
    arrived(((2, 1), 0), ((2, 1), 64), ((2, 3), 64), ((1, 2), 0), ((1, 2), 64), ((3, 2), 0), ((2, 2), 0), ((2, 2), 64))
    norms_of_plane(11, 16)
    multiply([0, 1, 2, 3, 4], 11, 16, first=True)
    arrived(("line", 4, 0), ("line", 4, 64))
    send_partner(4)
    arrived(("side", 4))
    send_partner_side(4)
    norms_of_line(3)
    norms_of_line(5)
    multiply([5, 6], 0, 16)

    gathers = list(copies.values())
    norms_of_line(4)
    for lo in (12, 8, 4, 0):
        multiply([7], lo, lo + 4)
        for at in reversed(range(lo, lo + 4)):
            rs_out[at] = side_by_side(y_acc[at * PTS : (at + 1) * PTS])
        group = []
        for at in reversed(range(lo, lo + 4)):
            dx, dy = PLANE[at]
            there = PLANE_AT[(-dx % NX, -dy % NY)]
            for c in range(2):
                to = partner if at == 0 else {**plane_peer(dx, dy), "core": 1}
                if at > 0 or c == 0:
                    group.append((c, describe(("part", c, there), rs_out.at[at], rs_in.at[c, there], to)))
        for c in range(2):

            @pl.when(core == c)
            def _():
                for whose, copy in group:
                    if whose == c:
                        copy.start()

    to_partner = describe("rows", owned.at[0], owned.at[0], partner)
    back = describe("back", g_sum.at[3], g_sum.at[3], partner)
    stages = []
    for stage, axis, size, landing in ((0, "x", NX, g_x), (1, "y", NY, g_y), (2, "z", NZ, g_z)):
        stages.append((stage, landing, [
            describe((axis, by), g_sum.at[stage], landing.at[by - 1], {axis: shift(axis, by, size)})
            for by in range(1, size)
        ]))

    def given(c):
        return [copies[("part", c, at)] for at in range(1 if c else 0, 16)]

    @pl.when(core == 0)
    def _():
        for copy in given(0):
            copy.wait_send()
        to_partner.wait_recv()
        back.wait_recv()

    @pl.when(core == 1)
    def _():
        totals = []
        for c in range(2):
            total = None if c == 0 else rs_out[0]
            for at in range(1 if c else 0, 16):
                copies[("part", c, at)].wait_recv()
                term = rs_in[c, at]
                total = term if total is None else total + term
            totals.append(total)
            owned[c] = total
            if c == 0:
                to_partner.start()
        sketched = jnp.concatenate([one_above_other(total) for total in totals], axis=0)
        tests = jnp.concatenate([tests_ref[1], tests_ref[0]], axis=0)
        products = high_dot(
            jnp.concatenate([tests, sketched], axis=1),
            jnp.concatenate([sketched, tests], axis=1),
            ((0,), (0,)),
        )
        top, bottom = products[:RANK], products[RANK:]
        turned = jnp.concatenate([top[:, RANK:], top[:, :RANK]], axis=1)
        lane = lax.broadcasted_iota(jnp.int32, bottom.shape, 1)
        g_sum[0] = jnp.where(lane < RANK, bottom, 0.5 * (bottom + turned))
        for stage, landing, group in stages:
            for copy in group:
                copy.start()
            value = g_sum[stage]
            for at, copy in enumerate(group):
                copy.wait_recv()
                value = value + landing[at]
            g_sum[stage + 1] = value
        back.start()
        for _, _, group in stages:
            for copy in group:
                copy.wait_send()
        for copy in given(1):
            copy.wait_send()
        to_partner.wait_send()
        back.wait_send()

    for copy in gathers:
        copy.wait_send()
    sketched = one_above_other(owned[core])
    both = g_sum[3]
    low = jnp.concatenate(inverses_of_cholesky([both[:, :RANK], both[:, RANK:]]), axis=0)
    both_ref[...] = high_dot(low, sketched, ((1,), (1,))) * math.sqrt(PTS * 256)
    assert len(copies) <= N_COPIES


def per_device(embeddings, sketch):
    vmem = pl.BlockSpec(memory_space=pltpu.VMEM)
    pair = (RANK, 2 * RANK)
    both = pl.pallas_call(
        kernel,
        out_shape=jax.ShapeDtypeStruct((2 * RANK, PTS), jnp.float32),
        in_specs=[vmem, vmem],
        out_specs=vmem,
        scratch_shapes=[
            pltpu.VMEM((NZ, 2 * PTS, WIDTH), jnp.bfloat16),
            pltpu.VMEM((16 * PTS, WIDTH), jnp.bfloat16),
            pltpu.VMEM((NZ, RANK + 16, 2 * PTS), jnp.bfloat16),
            pltpu.VMEM((NZ, 8, 2 * PTS), jnp.float32),
            pltpu.VMEM((16 * PTS, 128), jnp.float32),
            pltpu.VMEM((16 * PTS, RANK), jnp.float32),
            pltpu.VMEM((2, PTS, RANK), jnp.float32),
            pltpu.VMEM((16, PTS // 2, 2 * RANK), jnp.float32),
            pltpu.VMEM((2, 16, PTS // 2, 2 * RANK), jnp.float32),
            pltpu.VMEM((2, PTS // 2, 2 * RANK), jnp.float32),
            pltpu.VMEM((NX - 1, *pair), jnp.float32),
            pltpu.VMEM((NY - 1, *pair), jnp.float32),
            pltpu.VMEM((NZ - 1, *pair), jnp.float32),
            pltpu.VMEM((4, *pair), jnp.float32),
            pltpu.SemaphoreType.DMA((N_COPIES,)),
            pltpu.SemaphoreType.DMA((N_COPIES,)),
        ],
        compiler_params=pltpu.CompilerParams(
            collective_id=0, has_side_effects=True, vmem_limit_bytes=24 << 20
        ),
        name="nystrom",
    )(embeddings, sketch.T)
    return both[:RANK].T, both[RANK:].T


def solution(mesh):
    torus = Mesh(mesh.devices.reshape(NX, 2, NY, NZ), AXES)
    spec = P(AXES, None)
    return jax.shard_map(
        per_device, mesh=torus, in_specs=(spec, spec), out_specs=(spec, spec), check_vma=False
    )
```
